32 devices in a mesh: tok: 16 (over z, x, core), blk: 2 (over y).
Axes of the slice: x: 2, y: 2, z: 4, core: 2. Of those that a mesh axis runs over, the one named last changes fastest.
Arguments:
- activations: bfloat16 [2048, 7168], P('tok', 'blk'), may hold values from -600 to 600
- signs: float32 [7168], P('blk'), may hold values from -1 to 1, as said below
Outputs:
- hessian: float32 [7168, 7168], P('tok', 'blk')
- incoherence: float32 [7168], P('blk')
- largest_ratio: float32 [], replicated
The draws below stay inside these ranges and needn't reach their ends.
Inputs may be any that keep to these rules, and one draw needn't show every extreme that they name: `signs`: every entry is -1 or 1.
All inputs are finite; a program needn't handle non-finite values.
Results may differ from the reference program's by a relative error of at most 0.0037.
Values may be sent and summed in bfloat16 or wider, within the bound.
A program may use at most 640 MiB of HBM per device.

```python
import math
import jax
import jax.numpy as jnp
from jax import lax

WALSH = 512
MIX = 14
FEATURES = 7168
TOKENS = 2048


def draw_activations(key, part):
    noise_key, scale_key = jax.random.split(key, 2)
    position = jnp.arange(TOKENS, dtype=jnp.float32) / TOKENS
    ramp = jnp.exp(math.log(3.0) * position)[:, None]
    row_scale = jnp.exp(jax.random.uniform(scale_key, (TOKENS, 1), jnp.float32, 0.0, math.log(10.0)))
    values = jnp.clip(jax.random.normal(noise_key, (TOKENS, FEATURES), jnp.float32), -5.0, 5.0)
    return (values * ramp * row_scale).astype(jnp.bfloat16)


def draw_signs(key, part):
    coins = jax.random.randint(key, (FEATURES,), 0, 2)
    return (2 * coins - 1).astype(jnp.float32)


def setup_inputs(seed: int = 0) -> dict:
    seeds = jax.random.split(jax.random.key(seed), 3)
    return {
        "activations": draw_activations(jax.random.fold_in(seeds[2], 71), 0),
        "signs": draw_signs(jax.random.fold_in(seeds[2], 71), 0),
    }


EPS = 1e-06
DAMP = 0.01

def walsh_table(length):
    position = jnp.arange(length, dtype=jnp.int32)
    parity = jnp.zeros((length, length), jnp.int32)
    for bit_number in range(length.bit_length() - 1):
        parity = parity + (position[:, None] >> bit_number & 1) * (position[None, :] >> bit_number & 1)
    return (1 - 2 * (parity % 2)).astype(jnp.float32)

def cosine_table(length):
    rows_idx = jnp.arange(length, dtype=jnp.float32)[:, None]
    columns = jnp.arange(length, dtype=jnp.float32)[None, :]
    table = math.sqrt(2.0 / length) * jnp.cos(math.pi * (columns + 0.5) * rows_idx / length)
    return jnp.where(rows_idx == 0.0, table * math.sqrt(0.5), table)

def reference(activations, signs):
    signed = activations * signs.astype(jnp.bfloat16)[None, :]
    tokens_total = activations.shape[0]
    values = signed.astype(jnp.float32).reshape(tokens_total, WALSH, MIX)
    values = jnp.einsum('tba,ka->tbk', values, cosine_table(MIX), precision=lax.Precision.HIGHEST)
    values = jnp.einsum('tbk,cb->tck', values, walsh_table(WALSH) / math.sqrt(WALSH), precision=lax.Precision.HIGHEST)
    rotated = values.reshape(tokens_total, FEATURES).astype(jnp.bfloat16)
    gram_matrix = lax.dot_general(rotated, rotated, (((0,), (0,)), ((), ())), preferred_element_type=jnp.float32)
    on_diag = jnp.eye(FEATURES, dtype=jnp.bool_)
    trace_total = jnp.sum(jnp.diagonal(gram_matrix))
    diag_mean = trace_total / FEATURES + EPS
    hessian = gram_matrix / diag_mean + DAMP * on_diag.astype(jnp.float32)
    column_peak = lax.optimization_barrier(jnp.max(jnp.where(on_diag, 0.0, jnp.abs(gram_matrix)), axis=0))
    incoherence = column_peak / diag_mean
    return (hessian, incoherence, jnp.max(incoherence))
```

```python
import functools
import math

import jax
import jax.numpy as jnp
import numpy as np
from jax import lax
from jax.experimental import pallas as pl
from jax.experimental.pallas import tpu as pltpu
from jax.sharding import PartitionSpec as P

WALSH = 512
MIX = 14
FEATURES = 7168

EPS = 1e-06
DAMP = 0.01

LANES = 128
UNIT_WALSH = LANES // math.gcd(LANES, MIX)
UNIT = UNIT_WALSH * MIX


def parity(number):
    return bin(number).count("1") & 1


def unit_tables():
    walsh = np.array(
        [[1 - 2 * parity(i & j) for j in range(UNIT_WALSH)] for i in range(UNIT_WALSH)], np.float64
    )
    k = np.arange(MIX)[:, None]
    n = np.arange(MIX)[None, :]
    cosine = math.sqrt(2.0 / MIX) * np.cos(math.pi * (n + 0.5) * k / MIX)
    cosine[0] *= math.sqrt(0.5)
    table = np.kron(walsh, cosine.T).astype(np.float32)
    high = table.astype(jnp.bfloat16)
    low = (table - high.astype(np.float32)).astype(jnp.bfloat16)
    return high, low


def rotate_kernel(blocks, chunks, high_ref, low_ref, flips_ref, *refs):
    pieces, (out_ref, square_ref) = refs[:blocks], refs[blocks:]
    mixed = []
    for c in range(chunks):
        total = None
        for k in range(blocks):
            part = pieces[k][:, c * UNIT : (c + 1) * UNIT]
            value = jnp.dot(part, high_ref[...], preferred_element_type=jnp.float32)
            value += jnp.dot(part, low_ref[...], preferred_element_type=jnp.float32)
            value = value * flips_ref[0, k]
            total = value if total is None else total + value
        mixed.append(total)
    step = 1
    while step < chunks:
        for low in range(chunks):
            if not low & step:
                a, b = mixed[low], mixed[low | step]
                mixed[low], mixed[low | step] = a + b, a - b
        step *= 2
    square = jnp.float32(0.0)
    for c in range(chunks):
        rounded = (mixed[c] * (1.0 / math.sqrt(WALSH))).astype(jnp.bfloat16)
        out_ref[:, c * UNIT : (c + 1) * UNIT] = rounded
        wide = rounded.astype(jnp.float32)
        square += jnp.sum(wide * wide)
    square_ref[...] = jnp.full(square_ref.shape, square, jnp.float32)


def rotate(pieces, flips):
    blocks = len(pieces)
    rows, width = pieces[0].shape
    high, low = unit_tables()
    vmem = pl.BlockSpec(memory_space=pltpu.VMEM)
    return pl.pallas_call(
        functools.partial(rotate_kernel, blocks, width // UNIT),
        out_shape=(
            jax.ShapeDtypeStruct((rows, width), jnp.bfloat16),
            jax.ShapeDtypeStruct((8, LANES), jnp.float32),
        ),
        in_specs=[vmem, vmem, pl.BlockSpec(memory_space=pltpu.SMEM)] + [vmem] * blocks,
        out_specs=(vmem, vmem),
        compiler_params=pltpu.CompilerParams(vmem_limit_bytes=48 * 1024 * 1024),
        name="rotate",
    )(jnp.asarray(high), jnp.asarray(low), flips, *pieces)


def gram_kernel(rows, skew_ref, scale_ref, window_ref, columns_ref, hessian_ref, peak_ref, best):
    tile = pl.program_id(0)
    width = columns_ref.shape[1]
    skew = skew_ref[0, 0]
    diagonal = skew_ref[0, 1] - tile * width
    inverse = scale_ref[0, 0]
    block = lax.dot_general(
        window_ref[...], columns_ref[...], (((0,), (0,)), ((), ())), preferred_element_type=jnp.float32
    )
    whole = window_ref.shape[1]
    if whole == rows:
        block = block[:rows]
    else:
        other = whole - rows
        block = jnp.where(skew == 0, block[:rows], block[other:])
    row = lax.broadcasted_iota(jnp.int32, (rows, width), 0) + diagonal
    column = lax.broadcasted_iota(jnp.int32, (rows, width), 1)
    on_diag = row == column
    hessian_ref[...] = block * inverse + jnp.where(on_diag, DAMP, 0.0)
    size = jnp.where(on_diag, 0.0, jnp.abs(block))
    most = size[:, :LANES]
    for j in range(1, width // LANES):
        most = jnp.maximum(most, size[:, j * LANES : (j + 1) * LANES])

    @pl.when(tile == 0)
    def _():
        best[...] = most

    @pl.when(tile > 0)
    def _():
        best[...] = jnp.maximum(best[...], most)

    @pl.when(tile == pl.num_programs(0) - 1)
    def _():
        flat = jnp.max(best[...], axis=1, keepdims=True)
        turned = jnp.transpose(jnp.broadcast_to(flat, (rows, LANES)))
        peak_ref[...] = turned[:8] * inverse


def gram(window, columns, rows, skew, diagonal, inverse):
    tokens, width = columns.shape
    tile = 512 if width % 512 == 0 else LANES
    smem = pl.BlockSpec(memory_space=pltpu.SMEM)
    numbers = jnp.stack([skew, diagonal]).astype(jnp.int32).reshape(1, 2)
    return pl.pallas_call(
        functools.partial(gram_kernel, rows),
        grid=(width // tile,),
        out_shape=(
            jax.ShapeDtypeStruct((rows, width), jnp.float32),
            jax.ShapeDtypeStruct((8, rows), jnp.float32),
        ),
        in_specs=[
            smem,
            smem,
            pl.BlockSpec((tokens, window.shape[1]), lambda i: (0, 0)),
            pl.BlockSpec((tokens, tile), lambda i: (0, i)),
        ],
        out_specs=(
            pl.BlockSpec((rows, tile), lambda i: (0, i)),
            pl.BlockSpec((8, rows), lambda i: (0, 0)),
        ),
        scratch_shapes=[pltpu.VMEM((rows, LANES), jnp.float32)],
        compiler_params=pltpu.CompilerParams(vmem_limit_bytes=48 * 1024 * 1024),
        cost_estimate=pl.CostEstimate(
            flops=2 * rows * width * tokens,
            bytes_accessed=2 * tokens * width + 4 * rows * width,
            transcendentals=0,
        ),
        name="gram",
    )(numbers, inverse.reshape(1, 1), window, columns)


def per_device(activations, signs):
    tok_rows, block_width = activations.shape
    blocks = lax.axis_size("blk")
    me = lax.axis_index("blk")
    token_groups = lax.axis_size("tok")
    token_index = lax.axis_index("tok")
    signed = activations * signs.astype(jnp.bfloat16)[None, :]
    pieces, flips = [], []
    for k in range(blocks):
        piece = signed
        if k:
            piece = lax.ppermute(signed, "blk", [(i, i ^ k) for i in range(blocks)])
        pieces.append(piece)
        table = jnp.asarray([1.0 - 2.0 * parity(i & (i ^ k)) for i in range(blocks)], jnp.float32)
        flips.append(table[me])
    rotated, squares = rotate(pieces, jnp.stack(flips).reshape(1, blocks))
    trace_total = lax.psum(squares[0, 0], ("tok", "blk"))
    diag_mean = trace_total / FEATURES + EPS
    inverse = 1.0 / diag_mean

    row_count = FEATURES // token_groups
    window = -(-row_count // LANES) * LANES
    all_tokens = lax.all_gather(rotated, "tok", axis=0, tiled=True)
    first_row = token_index * row_count
    owner = first_row // block_width
    offset = first_row - owner * block_width
    start = jnp.minimum(offset // LANES * LANES, block_width - window)
    skew = offset - start
    own = lax.dynamic_slice_in_dim(all_tokens, start, window, 1)
    if blocks == 2:
        partner = lax.ppermute(own, "blk", [(0, 1), (1, 0)])
        rows_window = jnp.where(owner == me, own, partner)
    else:
        rows_window = lax.psum(jnp.where(owner == me, own, 0).astype(own.dtype), "blk")
    hessian, peak = gram(
        rows_window, all_tokens, row_count, skew, first_row - me * block_width, inverse
    )
    peaks = lax.all_gather(peak[0], ("blk", "tok"), axis=0).reshape(blocks, FEATURES)
    ratios = jnp.max(peaks, axis=0)
    incoherence = lax.dynamic_slice_in_dim(ratios, me * block_width, block_width, 0)
    return (hessian, incoherence, jnp.max(ratios))


def solution(mesh):
    in_specs = (P("tok", "blk"), P("blk"))
    out_specs = (P("tok", "blk"), P("blk"), P())
    return jax.shard_map(
        per_device, mesh=mesh, in_specs=in_specs, out_specs=out_specs, check_vma=False
    )
```

```python
import functools
import math

import jax
import jax.numpy as jnp
import numpy as np
from jax import lax
from jax.experimental import pallas as pl
from jax.experimental.pallas import tpu as pltpu
from jax.sharding import PartitionSpec as P

WALSH = 512
MIX = 14
FEATURES = 7168

EPS = 1e-06
DAMP = 0.01

LANES = 128
UNIT_WALSH = LANES // math.gcd(LANES, MIX)
UNIT = UNIT_WALSH * MIX
MESH = pl.DeviceIdType.MESH


def parity(number):
    return bin(number).count("1") & 1


def unit_tables():
    walsh = np.array(
        [[1 - 2 * parity(i & j) for j in range(UNIT_WALSH)] for i in range(UNIT_WALSH)], np.float64
    )
    k = np.arange(MIX)[:, None]
    n = np.arange(MIX)[None, :]
    cosine = math.sqrt(2.0 / MIX) * np.cos(math.pi * (n + 0.5) * k / MIX)
    cosine[0] *= math.sqrt(0.5)
    table = np.kron(walsh, cosine.T).astype(np.float32)
    high = table.astype(jnp.bfloat16)
    low = (table - high.astype(np.float32)).astype(jnp.bfloat16)
    return high, low


def rotate_kernel(blocks, chunks, high_ref, low_ref, flips_ref, *refs):
    pieces, (out_ref, square_ref) = refs[:blocks], refs[blocks:]
    mixed = []
    for c in range(chunks):
        total = None
        for k in range(blocks):
            part = pieces[k][:, c * UNIT : (c + 1) * UNIT]
            value = jnp.dot(part, high_ref[...], preferred_element_type=jnp.float32)
            value += jnp.dot(part, low_ref[...], preferred_element_type=jnp.float32)
            value = value * flips_ref[0, k]
            total = value if total is None else total + value
        mixed.append(total)
    step = 1
    while step < chunks:
        for low in range(chunks):
            if not low & step:
                a, b = mixed[low], mixed[low | step]
                mixed[low], mixed[low | step] = a + b, a - b
        step *= 2
    square = jnp.float32(0.0)
    for c in range(chunks):
        rounded = (mixed[c] * (1.0 / math.sqrt(WALSH))).astype(jnp.bfloat16)
        out_ref[:, c * UNIT : (c + 1) * UNIT] = rounded
        wide = rounded.astype(jnp.float32)
        square += jnp.sum(wide * wide)
    square_ref[...] = jnp.full(square_ref.shape, square, jnp.float32)


def rotate(pieces, flips):
    blocks = len(pieces)
    rows, width = pieces[0].shape
    high, low = unit_tables()
    vmem = pl.BlockSpec(memory_space=pltpu.VMEM)
    return pl.pallas_call(
        functools.partial(rotate_kernel, blocks, width // UNIT),
        out_shape=(
            jax.ShapeDtypeStruct((rows, width), jnp.bfloat16),
            jax.ShapeDtypeStruct((8, LANES), jnp.float32),
        ),
        in_specs=[vmem, vmem, pl.BlockSpec(memory_space=pltpu.SMEM)] + [vmem] * blocks,
        out_specs=(vmem, vmem),
        compiler_params=pltpu.CompilerParams(vmem_limit_bytes=48 * 1024 * 1024),
        name="rotate",
    )(jnp.asarray(high), jnp.asarray(low), flips, *pieces)


def place(tok, row_count, width, window):
    first = tok * row_count
    owner = first // width
    offset = first - owner * width
    start = jnp.minimum(offset // LANES * LANES, width - window)
    return owner, start, offset - start


def greet_all(tok, blk):
    tokens, blocks = lax.axis_size("tok"), lax.axis_size("blk")
    count = tokens * blocks
    barrier = pltpu.get_barrier_semaphore()
    me = tok * blocks + blk

    @pl.loop(1, count)
    def _(k):
        other = lax.rem(me + k, count)
        pl.semaphore_signal(
            barrier, inc=1, device_id={"tok": other // blocks, "blk": other % blocks}, device_id_type=MESH
        )

    pl.semaphore_wait(barrier, count - 1)


def broadcast_start(tok, blk, src, dst, send, recv):
    tokens, blocks = lax.axis_size("tok"), lax.axis_size("blk")
    count = tokens * blocks
    me = tok * blocks + blk

    @pl.loop(1, count)
    def _(k):
        other = lax.rem(me + k, count)
        pltpu.make_async_remote_copy(
            src, dst.at[me], send, recv,
            device_id={"tok": other // blocks, "blk": other % blocks}, device_id_type=MESH,
        ).start()


def broadcast_wait(tok, blk, dst, send, recv):
    count = dst.shape[0] - 1
    both = pltpu.make_async_remote_copy(
        dst.at[pl.ds(0, count)], dst.at[pl.ds(0, count)], send, recv,
        device_id={"tok": tok, "blk": blk}, device_id_type=MESH,
    )
    both.wait_send()
    both.wait_recv()


def spread_kernel(src, dst, local, send, recv):
    tok, blk = lax.axis_index("tok"), lax.axis_index("blk")
    greet_all(tok, blk)
    broadcast_start(tok, blk, src, dst, send, recv)
    own = pltpu.make_async_copy(src, dst.at[tok * lax.axis_size("blk") + blk], local)
    own.start()
    own.wait()
    broadcast_wait(tok, blk, dst, send, recv)


def spread(block):
    count = lax.axis_size("tok") * lax.axis_size("blk")
    vmem = pl.BlockSpec(memory_space=pltpu.VMEM)
    return pl.pallas_call(
        spread_kernel,
        out_shape=jax.ShapeDtypeStruct((count,) + block.shape, block.dtype),
        in_specs=[vmem],
        out_specs=vmem,
        scratch_shapes=[pltpu.SemaphoreType.DMA] * 3,
        compiler_params=pltpu.CompilerParams(collective_id=1, has_side_effects=True),
        name="spread",
    )(block)


def gather_kernel(
    depth, across, sub, early, row_count, rot, part, cols, rows, parts,
    local, recv, pair_send, pair_recv, z_send, x_send, y_send, y_recv, part_local, part_send, part_recv,
):
    tok, blk = lax.axis_index("tok"), lax.axis_index("blk")
    blocks = lax.axis_size("blk")
    tok_rows, width = rot.shape
    window = rows.shape[1]
    half = cols.shape[0] // 2
    steps = tok_rows // sub
    core, chip = tok % 2, tok // 2
    z, x = chip // across, chip % across

    greet_all(tok, blk)
    own_rows = pltpu.make_async_copy(rot, cols.at[pl.ds(pl.multiple_of(tok * tok_rows, sub), tok_rows)], local)
    own_rows.start()

    def first_row(oz, ox, s):
        return pl.multiple_of(((oz * across + ox) * 2 + core) * tok_rows + s * sub, sub)

    def remote(src, dst, send, arrive, to_tok, to_blk):
        return pltpu.make_async_remote_copy(
            src, dst, send, arrive, device_id={"tok": to_tok, "blk": to_blk}, device_id_type=MESH
        )

    def fan(src, oz, ox, s, z_ways, x_ways):
        row = first_row(oz, ox, s)
        dst = cols.at[pl.ds(row, sub)]
        arrive = recv.at[(oz * across + ox) * steps + s]
        for way in x_ways:

            @pl.when((x + way >= 0) & (x + way < across))
            def _():
                remote(src, dst, x_send.at[(way + 1) // 2], arrive, tok + 2 * way, blk).start()

        for way in z_ways:

            @pl.when((z + way >= 0) & (z + way < depth))
            def _():
                remote(src, dst, z_send.at[(way + 1) // 2], arrive, tok + 2 * across * way, blk).start()

        remote(src, dst, pair_send, pair_recv, tok + 1 - 2 * core, blk).start()
        for j in range(2):
            owner, start, _ = place(chip * 2 + j, row_count, width, window)

            @pl.when(owner == blk)
            def _():
                part_src = src.at[:, pl.ds(pl.multiple_of(start, LANES), window)]
                for k in range(1, blocks):
                    remote(
                        part_src, rows.at[pl.ds(row, sub)], y_send.at[2 * k + j], y_recv,
                        chip * 2 + j, lax.rem(blk + k, blocks),
                    ).start()

    def relay(oz, ox, s, z_ways, x_ways):
        piece = cols.at[pl.ds(first_row(oz, ox, s), sub)]
        remote(piece, piece, pair_send, recv.at[(oz * across + ox) * steps + s], tok, blk).wait_recv()
        fan(piece, oz, ox, s, z_ways, x_ways)

    @pl.loop(0, steps)
    def _(s):
        fan(rot.at[pl.ds(pl.multiple_of(s * sub, sub), sub)], z, x, s, (1, -1), (1, -1))

    broadcast_start(tok, blk, part, parts, part_send, part_recv)
    own_part = pltpu.make_async_copy(part, parts.at[tok * blocks + blk], part_local)
    own_part.start()

    for dx in range(1, across):
        for way in (1, -1):
            ox = x - way * dx

            @pl.when((ox >= 0) & (ox < across))
            def _():
                for s in range(early):
                    relay(z, ox, s, (1, -1), (way,))

    for dz in range(1, depth):

        @pl.loop(early, steps)
        def _(s):
            for way in (1, -1):
                oz = z - way * dz

                @pl.when((oz >= 0) & (oz < depth))
                def _():
                    relay(oz, x, s, (way,), (1, -1))

        for way in (1, -1):
            oz = z - way * dz

            @pl.when((oz >= 0) & (oz < depth))
            def _():
                @pl.loop(0, across * early)
                def _(n):
                    relay(oz, n // early, n % early, (way,), ())

    for dx in range(1, across):
        for way in (1, -1):
            ox = x - way * dx

            @pl.when((ox >= 0) & (ox < across))
            def _():
                for dz in range(depth):
                    for side in (1, -1) if dz else (1,):
                        oz = z - side * dz

                        @pl.when((oz >= 0) & (oz < depth))
                        def _():
                            @pl.loop(early, steps)
                            def _(s):
                                relay(oz, ox, s, (), (way,))

    def settle(count, send):
        piece = cols.at[pl.ds(0, count)]
        remote(piece, piece, send, pair_recv, tok, blk).wait_send()

    late = steps - early
    for v in range(depth):
        @pl.when(z == v)
        def _():
            unit = (late + early * across) * sub
            if v < depth - 1:
                settle((v + 1) * unit, z_send.at[1])
            if v > 0:
                settle((depth - v) * unit, z_send.at[0])

    for v in range(across):
        @pl.when(x == v)
        def _():
            unit = (late * depth + early) * sub
            if v < across - 1:
                settle((v + 1) * unit, x_send.at[1])
            if v > 0:
                settle((across - v) * unit, x_send.at[0])

    settle(half, pair_send)
    for j in range(2):
        owner, _, _ = place(chip * 2 + j, row_count, width, window)

        @pl.when(owner == blk)
        def _():
            piece = rows.at[pl.ds(0, half)]
            for k in range(1, blocks):
                remote(piece, piece, y_send.at[2 * k + j], y_recv, tok, blk).wait_send()

    piece = cols.at[pl.ds(0, half)]
    remote(piece, piece, pair_send, pair_recv, tok, blk).wait_recv()
    owner, _, _ = place(tok, row_count, width, window)

    @pl.when(owner != blk)
    def _():
        remote(rows, rows, pair_send, y_recv, tok, blk).wait_recv()

    own_rows.wait()
    own_part.wait()
    broadcast_wait(tok, blk, parts, part_send, part_recv)


def gather(rotated, squares, window, row_count):
    tok_rows, width = rotated.shape
    groups, blocks = lax.axis_size("tok"), lax.axis_size("blk")
    depth = 4 if groups % 8 == 0 else 1
    across = groups // (2 * depth)
    sub = 16
    steps = tok_rows // sub
    dma = pltpu.SemaphoreType.DMA
    vmem = pl.BlockSpec(memory_space=pltpu.VMEM)
    anywhere = pl.BlockSpec(memory_space=pl.ANY)
    return pl.pallas_call(
        functools.partial(gather_kernel, depth, across, sub, 1, row_count),
        out_shape=(
            jax.ShapeDtypeStruct((groups * tok_rows, width), rotated.dtype),
            jax.ShapeDtypeStruct((groups * tok_rows, window), rotated.dtype),
            jax.ShapeDtypeStruct((groups * blocks,) + squares.shape, squares.dtype),
        ),
        in_specs=[vmem, vmem],
        out_specs=(anywhere, anywhere, vmem),
        scratch_shapes=[
            dma, dma((groups // 2 * steps,)), dma, dma, dma((2,)), dma((2,)), dma((2 * blocks,)), dma,
            dma, dma, dma,
        ],
        compiler_params=pltpu.CompilerParams(
            collective_id=0, has_side_effects=True, vmem_limit_bytes=16 * 1024 * 1024
        ),
        name="gather",
    )(rotated, squares)


def gram_kernel(rows, scale_ref, window_ref, all_ref, columns_ref, hessian_ref, peak_ref, best, left, sem):
    tile = pl.program_id(0)
    width = columns_ref.shape[1]
    tok, blk = lax.axis_index("tok"), lax.axis_index("blk")
    whole = window_ref.shape[1]
    block_width = all_ref.shape[1]
    owner, start, skew = place(tok, rows, block_width, whole)
    diagonal = tok * rows - blk * block_width - tile * width
    inverse = scale_ref[0, 0]

    @pl.when((tile == 0) & (owner == blk))
    def _():
        own = pltpu.make_async_copy(all_ref.at[:, pl.ds(pl.multiple_of(start, LANES), whole)], left, sem)
        own.start()
        own.wait()

    @pl.when((tile == 0) & (owner != blk))
    def _():
        given = pltpu.make_async_copy(window_ref, left, sem)
        given.start()
        given.wait()

    block = lax.dot_general(
        left[...], columns_ref[...], (((0,), (0,)), ((), ())), preferred_element_type=jnp.float32
    )
    if whole == rows:
        block = block[:rows]
    else:
        block = jnp.where(skew == 0, block[:rows], block[whole - rows :])
    row = lax.broadcasted_iota(jnp.int32, (rows, width), 0) + diagonal
    column = lax.broadcasted_iota(jnp.int32, (rows, width), 1)
    on_diag = row == column
    hessian_ref[...] = block * inverse + jnp.where(on_diag, DAMP, 0.0)
    size = jnp.where(on_diag, 0.0, jnp.abs(block))
    most = size[:, :LANES]
    for j in range(1, width // LANES):
        most = jnp.maximum(most, size[:, j * LANES : (j + 1) * LANES])

    @pl.when(tile == 0)
    def _():
        best[...] = most

    @pl.when(tile > 0)
    def _():
        best[...] = jnp.maximum(best[...], most)

    @pl.when(tile == pl.num_programs(0) - 1)
    def _():
        flat = jnp.max(best[...], axis=1, keepdims=True)
        turned = jnp.transpose(jnp.broadcast_to(flat, (rows, LANES)))
        peak_ref[...] = turned[:8] * inverse


def gram(window, columns, rows, inverse):
    tokens, width = columns.shape
    tile = 512 if width % 512 == 0 else LANES
    anywhere = pl.BlockSpec(memory_space=pl.ANY)
    return pl.pallas_call(
        functools.partial(gram_kernel, rows),
        grid=(width // tile,),
        out_shape=(
            jax.ShapeDtypeStruct((rows, width), jnp.float32),
            jax.ShapeDtypeStruct((8, rows), jnp.float32),
        ),
        in_specs=[
            pl.BlockSpec(memory_space=pltpu.SMEM),
            anywhere,
            anywhere,
            pl.BlockSpec((tokens, tile), lambda i: (0, i)),
        ],
        out_specs=(
            pl.BlockSpec((rows, tile), lambda i: (0, i)),
            pl.BlockSpec((8, rows), lambda i: (0, 0)),
        ),
        scratch_shapes=[
            pltpu.VMEM((rows, LANES), jnp.float32),
            pltpu.VMEM(window.shape, window.dtype),
            pltpu.SemaphoreType.DMA,
        ],
        compiler_params=pltpu.CompilerParams(vmem_limit_bytes=48 * 1024 * 1024),
        cost_estimate=pl.CostEstimate(
            flops=2 * rows * width * tokens,
            bytes_accessed=2 * tokens * width + 4 * rows * width,
            transcendentals=0,
        ),
        name="gram",
    )(inverse.reshape(1, 1), window, columns, columns)


def per_device(activations, signs):
    tok_rows, block_width = activations.shape
    blocks = lax.axis_size("blk")
    me = lax.axis_index("blk")
    token_groups = lax.axis_size("tok")
    signed = activations * signs.astype(jnp.bfloat16)[None, :]
    pieces, flips = [], []
    for k in range(blocks):
        piece = signed
        if k:
            piece = lax.ppermute(signed, "blk", [(i, i ^ k) for i in range(blocks)])
        pieces.append(piece)
        table = jnp.asarray([1.0 - 2.0 * parity(i & (i ^ k)) for i in range(blocks)], jnp.float32)
        flips.append(table[me])
    rotated, squares = rotate(pieces, jnp.stack(flips).reshape(1, blocks))
    row_count = FEATURES // token_groups
    window = -(-row_count // LANES) * LANES
    all_tokens, rows_window, parts = gather(rotated, squares, window, row_count)
    trace_total = jnp.sum(parts[:, 0, 0])
    diag_mean = trace_total / FEATURES + EPS
    hessian, peak = gram(rows_window, all_tokens, row_count, 1.0 / diag_mean)
    peaks = spread(peak)[:, 0, :]
    ratios = jnp.max(peaks.reshape(token_groups, blocks, row_count), axis=1).reshape(FEATURES)
    incoherence = lax.dynamic_slice_in_dim(ratios, me * block_width, block_width, 0)
    return (hessian, incoherence, jnp.max(ratios))


def solution(mesh):
    in_specs = (P("tok", "blk"), P("blk"))
    out_specs = (P("tok", "blk"), P("blk"), P())
    return jax.shard_map(
        per_device, mesh=mesh, in_specs=in_specs, out_specs=out_specs, check_vma=False
    )
```

```python
import functools
import math

import jax
import jax.numpy as jnp
import numpy as np
from jax import lax
from jax.experimental import pallas as pl
from jax.experimental.pallas import tpu as pltpu
from jax.sharding import PartitionSpec as P

WALSH = 512
MIX = 14
FEATURES = 7168

EPS = 1e-06
DAMP = 0.01

LANES = 128
UNIT_WALSH = LANES // math.gcd(LANES, MIX)
UNIT = UNIT_WALSH * MIX
MESH = pl.DeviceIdType.MESH


def parity(number):
    return bin(number).count("1") & 1


def unit_tables():
    walsh = np.array(
        [[1 - 2 * parity(i & j) for j in range(UNIT_WALSH)] for i in range(UNIT_WALSH)], np.float64
    )
    k = np.arange(MIX)[:, None]
    n = np.arange(MIX)[None, :]
    cosine = math.sqrt(2.0 / MIX) * np.cos(math.pi * (n + 0.5) * k / MIX)
    cosine[0] *= math.sqrt(0.5)
    table = np.kron(walsh, cosine.T).astype(np.float32)
    high = table.astype(jnp.bfloat16)
    low = (table - high.astype(np.float32)).astype(jnp.bfloat16)
    return high, low


def rotate_kernel(blocks, chunks, high_ref, low_ref, flips_ref, *refs):
    pieces, (out_ref, square_ref) = refs[:blocks], refs[blocks:]
    mixed = []
    for c in range(chunks):
        total = None
        for k in range(blocks):
            part = pieces[k][:, c * UNIT : (c + 1) * UNIT]
            value = jnp.dot(part, high_ref[...], preferred_element_type=jnp.float32)
            value += jnp.dot(part, low_ref[...], preferred_element_type=jnp.float32)
            value = value * flips_ref[0, k]
            total = value if total is None else total + value
        mixed.append(total)
    step = 1
    while step < chunks:
        for low in range(chunks):
            if not low & step:
                a, b = mixed[low], mixed[low | step]
                mixed[low], mixed[low | step] = a + b, a - b
        step *= 2
    square = jnp.float32(0.0)
    for c in range(chunks):
        rounded = (mixed[c] * (1.0 / math.sqrt(WALSH))).astype(jnp.bfloat16)
        out_ref[:, c * UNIT : (c + 1) * UNIT] = rounded
        wide = rounded.astype(jnp.float32)
        square += jnp.sum(wide * wide)
    square_ref[...] = jnp.full(square_ref.shape, square, jnp.float32)


def rotate(pieces, flips):
    blocks = len(pieces)
    rows, width = pieces[0].shape
    high, low = unit_tables()
    vmem = pl.BlockSpec(memory_space=pltpu.VMEM)
    return pl.pallas_call(
        functools.partial(rotate_kernel, blocks, width // UNIT),
        out_shape=(
            jax.ShapeDtypeStruct((rows, width), jnp.bfloat16),
            jax.ShapeDtypeStruct((8, LANES), jnp.float32),
        ),
        in_specs=[vmem, vmem, pl.BlockSpec(memory_space=pltpu.SMEM)] + [vmem] * blocks,
        out_specs=(vmem, vmem),
        compiler_params=pltpu.CompilerParams(vmem_limit_bytes=48 * 1024 * 1024),
        name="rotate",
    )(jnp.asarray(high), jnp.asarray(low), flips, *pieces)


def place(tok, row_count, width, window):
    first = tok * row_count
    owner = first // width
    offset = first - owner * width
    start = jnp.minimum(offset // LANES * LANES, width - window)
    return owner, start, offset - start


def greet_all(tok, blk):
    tokens, blocks = lax.axis_size("tok"), lax.axis_size("blk")
    count = tokens * blocks
    barrier = pltpu.get_barrier_semaphore()
    me = tok * blocks + blk

    @pl.loop(1, count)
    def _(k):
        other = lax.rem(me + k, count)
        pl.semaphore_signal(
            barrier, inc=1, device_id={"tok": other // blocks, "blk": other % blocks}, device_id_type=MESH
        )

    pl.semaphore_wait(barrier, count - 1)


def broadcast_start(tok, blk, src, dst, send, recv):
    tokens, blocks = lax.axis_size("tok"), lax.axis_size("blk")
    count = tokens * blocks
    me = tok * blocks + blk

    @pl.loop(1, count)
    def _(k):
        other = lax.rem(me + k, count)
        pltpu.make_async_remote_copy(
            src, dst.at[me], send, recv,
            device_id={"tok": other // blocks, "blk": other % blocks}, device_id_type=MESH,
        ).start()


def broadcast_wait(tok, blk, dst, send, recv):
    count = dst.shape[0] - 1
    both = pltpu.make_async_remote_copy(
        dst.at[pl.ds(0, count)], dst.at[pl.ds(0, count)], send, recv,
        device_id={"tok": tok, "blk": blk}, device_id_type=MESH,
    )
    both.wait_send()
    both.wait_recv()


def spread_kernel(src, dst, local, send, recv):
    tok, blk = lax.axis_index("tok"), lax.axis_index("blk")
    greet_all(tok, blk)
    broadcast_start(tok, blk, src, dst, send, recv)
    own = pltpu.make_async_copy(src, dst.at[tok * lax.axis_size("blk") + blk], local)
    own.start()
    own.wait()
    broadcast_wait(tok, blk, dst, send, recv)


def spread(block):
    count = lax.axis_size("tok") * lax.axis_size("blk")
    vmem = pl.BlockSpec(memory_space=pltpu.VMEM)
    return pl.pallas_call(
        spread_kernel,
        out_shape=jax.ShapeDtypeStruct((count,) + block.shape, block.dtype),
        in_specs=[vmem],
        out_specs=vmem,
        scratch_shapes=[pltpu.SemaphoreType.DMA] * 3,
        compiler_params=pltpu.CompilerParams(collective_id=1, has_side_effects=True),
        name="spread",
    )(block)


def gather_kernel(
    depth, across, sub, early, row_count, rot, part, cols, rows, parts,
    local, recv, pair_send, pair_recv, z_send, x_send, y_send, y_recv, part_local, part_send, part_recv,
):
    tok, blk = lax.axis_index("tok"), lax.axis_index("blk")
    blocks = lax.axis_size("blk")
    tok_rows, width = rot.shape
    window = rows.shape[1]
    half = cols.shape[0] // 2
    steps = tok_rows // sub
    core, chip = tok % 2, tok // 2
    z, x = chip // across, chip % across

    greet_all(tok, blk)
    own_rows = pltpu.make_async_copy(rot, cols.at[pl.ds(pl.multiple_of(tok * tok_rows, sub), tok_rows)], local)
    own_rows.start()

    def first_row(oz, ox, s):
        return pl.multiple_of(((oz * across + ox) * 2 + core) * tok_rows + s * sub, sub)

    def remote(src, dst, send, arrive, to_tok, to_blk):
        return pltpu.make_async_remote_copy(
            src, dst, send, arrive, device_id={"tok": to_tok, "blk": to_blk}, device_id_type=MESH
        )

    def fan(src, oz, ox, s, z_ways, x_ways):
        row = first_row(oz, ox, s)
        dst = cols.at[pl.ds(row, sub)]
        arrive = recv.at[(oz * across + ox) * steps + s]
        for way in x_ways:

            @pl.when((x + way >= 0) & (x + way < across))
            def _():
                remote(src, dst, x_send.at[(way + 1) // 2], arrive, tok + 2 * way, blk).start()

        for way in z_ways:

            @pl.when((z + way >= 0) & (z + way < depth))
            def _():
                remote(src, dst, z_send.at[(way + 1) // 2], arrive, tok + 2 * across * way, blk).start()

        remote(src, dst, pair_send, pair_recv, tok + 1 - 2 * core, blk).start()
        for j in range(2):
            owner, start, _ = place(chip * 2 + j, row_count, width, window)

            @pl.when(owner == blk)
            def _():
                part_src = src.at[:, pl.ds(pl.multiple_of(start, LANES), window)]
                for k in range(1, blocks):
                    remote(
                        part_src, rows.at[pl.ds(row, sub)], y_send.at[2 * k + j], y_recv,
                        chip * 2 + j, lax.rem(blk + k, blocks),
                    ).start()

    def relay(oz, ox, s, z_ways, x_ways):
        piece = cols.at[pl.ds(first_row(oz, ox, s), sub)]
        remote(piece, piece, pair_send, recv.at[(oz * across + ox) * steps + s], tok, blk).wait_recv()
        fan(piece, oz, ox, s, z_ways, x_ways)

    @pl.loop(0, steps)
    def _(s):
        fan(rot.at[pl.ds(pl.multiple_of(s * sub, sub), sub)], z, x, s, (1, -1), (1, -1))

    broadcast_start(tok, blk, part, parts, part_send, part_recv)
    own_part = pltpu.make_async_copy(part, parts.at[tok * blocks + blk], part_local)
    own_part.start()

    for dx in range(1, across):
        for way in (1, -1):
            ox = x - way * dx

            @pl.when((ox >= 0) & (ox < across))
            def _():
                for s in range(early):
                    relay(z, ox, s, (1, -1), (way,))

    for dz in range(1, depth):

        @pl.loop(early, steps)
        def _(s):
            for way in (1, -1):
                oz = z - way * dz

                @pl.when((oz >= 0) & (oz < depth))
                def _():
                    relay(oz, x, s, (way,), (1, -1))

        for way in (1, -1):
            oz = z - way * dz

            @pl.when((oz >= 0) & (oz < depth))
            def _():
                @pl.loop(0, across * early)
                def _(n):
                    relay(oz, n // early, n % early, (way,), ())

    for dx in range(1, across):
        for way in (1, -1):
            ox = x - way * dx

            @pl.when((ox >= 0) & (ox < across))
            def _():
                for dz in range(depth):
                    for side in (1, -1) if dz else (1,):
                        oz = z - side * dz

                        @pl.when((oz >= 0) & (oz < depth))
                        def _():
                            @pl.loop(early, steps)
                            def _(s):
                                relay(oz, ox, s, (), (way,))

    def settle(count, send):
        piece = cols.at[pl.ds(0, count)]
        remote(piece, piece, send, pair_recv, tok, blk).wait_send()

    late = steps - early
    for v in range(depth):
        @pl.when(z == v)
        def _():
            unit = (late + early * across) * sub
            if v < depth - 1:
                settle((v + 1) * unit, z_send.at[1])
            if v > 0:
                settle((depth - v) * unit, z_send.at[0])

    for v in range(across):
        @pl.when(x == v)
        def _():
            unit = (late * depth + early) * sub
            if v < across - 1:
                settle((v + 1) * unit, x_send.at[1])
            if v > 0:
                settle((across - v) * unit, x_send.at[0])

    settle(half, pair_send)
    for j in range(2):
        owner, _, _ = place(chip * 2 + j, row_count, width, window)

        @pl.when(owner == blk)
        def _():
            piece = rows.at[pl.ds(0, half)]
            for k in range(1, blocks):
                remote(piece, piece, y_send.at[2 * k + j], y_recv, tok, blk).wait_send()

    piece = cols.at[pl.ds(0, half)]
    remote(piece, piece, pair_send, pair_recv, tok, blk).wait_recv()
    owner, _, _ = place(tok, row_count, width, window)

    @pl.when(owner != blk)
    def _():
        remote(rows, rows, pair_send, y_recv, tok, blk).wait_recv()

    own_rows.wait()
    own_part.wait()
    broadcast_wait(tok, blk, parts, part_send, part_recv)


def gather(rotated, squares, window, row_count):
    tok_rows, width = rotated.shape
    groups, blocks = lax.axis_size("tok"), lax.axis_size("blk")
    depth = 4 if groups % 8 == 0 else 1
    across = groups // (2 * depth)
    sub = 16
    steps = tok_rows // sub
    dma = pltpu.SemaphoreType.DMA
    vmem = pl.BlockSpec(memory_space=pltpu.VMEM)
    anywhere = pl.BlockSpec(memory_space=pl.ANY)
    return pl.pallas_call(
        functools.partial(gather_kernel, depth, across, sub, 1, row_count),
        out_shape=(
            jax.ShapeDtypeStruct((groups * tok_rows, width), rotated.dtype),
            jax.ShapeDtypeStruct((groups * tok_rows, window), rotated.dtype),
            jax.ShapeDtypeStruct((groups * blocks,) + squares.shape, squares.dtype),
        ),
        in_specs=[vmem, vmem],
        out_specs=(anywhere, anywhere, vmem),
        scratch_shapes=[
            dma, dma((groups // 2 * steps,)), dma, dma, dma((2,)), dma((2,)), dma((2 * blocks,)), dma,
            dma, dma, dma,
        ],
        compiler_params=pltpu.CompilerParams(
            collective_id=0, has_side_effects=True, vmem_limit_bytes=16 * 1024 * 1024
        ),
        name="gather",
    )(rotated, squares)


def gram_kernel(rows, scale_ref, window_ref, all_ref, columns_ref, hessian_ref, peak_ref, best, left, turned_left, sem):
    tile = pl.program_id(0)
    width = columns_ref.shape[1]
    tok, blk = lax.axis_index("tok"), lax.axis_index("blk")
    whole = window_ref.shape[1]
    block_width = all_ref.shape[1]
    owner, start, skew = place(tok, rows, block_width, whole)
    diagonal = tok * rows - blk * block_width - tile * width
    inverse = scale_ref[0, 0]

    @pl.when((tile == 0) & (owner == blk))
    def _():
        own = pltpu.make_async_copy(all_ref.at[:, pl.ds(pl.multiple_of(start, LANES), whole)], left, sem)
        own.start()
        own.wait()

    @pl.when((tile == 0) & (owner != blk))
    def _():
        given = pltpu.make_async_copy(window_ref, left, sem)
        given.start()
        given.wait()

    @pl.when(tile == 0)
    def _():
        turned_left[...] = jnp.transpose(left[...])

    block = jnp.dot(turned_left[...], columns_ref[...], preferred_element_type=jnp.float32)
    if whole == rows:
        block = block[:rows]
    else:
        block = jnp.where(skew == 0, block[:rows], block[whole - rows :])
    row = lax.broadcasted_iota(jnp.int32, (rows, width), 0) + diagonal
    column = lax.broadcasted_iota(jnp.int32, (rows, width), 1)
    on_diag = row == column
    hessian_ref[...] = block * inverse + jnp.where(on_diag, DAMP, 0.0)
    size = jnp.where(on_diag, 0.0, jnp.abs(block))
    most = size[:, :LANES]
    for j in range(1, width // LANES):
        most = jnp.maximum(most, size[:, j * LANES : (j + 1) * LANES])

    @pl.when(tile == 0)
    def _():
        best[...] = most

    @pl.when(tile > 0)
    def _():
        best[...] = jnp.maximum(best[...], most)

    @pl.when(tile == pl.num_programs(0) - 1)
    def _():
        flat = jnp.max(best[...], axis=1, keepdims=True)
        turned = jnp.transpose(jnp.broadcast_to(flat, (rows, LANES)))
        peak_ref[...] = turned[:8] * inverse


def gram(window, columns, rows, inverse):
    tokens, width = columns.shape
    tile = 512 if width % 512 == 0 else LANES
    anywhere = pl.BlockSpec(memory_space=pl.ANY)
    return pl.pallas_call(
        functools.partial(gram_kernel, rows),
        grid=(width // tile,),
        out_shape=(
            jax.ShapeDtypeStruct((rows, width), jnp.float32),
            jax.ShapeDtypeStruct((8, rows), jnp.float32),
        ),
        in_specs=[
            pl.BlockSpec(memory_space=pltpu.SMEM),
            anywhere,
            anywhere,
            pl.BlockSpec((tokens, tile), lambda i: (0, i)),
        ],
        out_specs=(
            pl.BlockSpec((rows, tile), lambda i: (0, i)),
            pl.BlockSpec((8, rows), lambda i: (0, 0)),
        ),
        scratch_shapes=[
            pltpu.VMEM((rows, LANES), jnp.float32),
            pltpu.VMEM(window.shape, window.dtype),
            pltpu.VMEM(window.shape[::-1], window.dtype),
            pltpu.SemaphoreType.DMA,
        ],
        compiler_params=pltpu.CompilerParams(vmem_limit_bytes=60 * 1024 * 1024),
        cost_estimate=pl.CostEstimate(
            flops=2 * rows * width * tokens,
            bytes_accessed=2 * tokens * width + 4 * rows * width,
            transcendentals=0,
        ),
        name="gram",
    )(inverse.reshape(1, 1), window, columns, columns)


def per_device(activations, signs):
    tok_rows, block_width = activations.shape
    blocks = lax.axis_size("blk")
    me = lax.axis_index("blk")
    token_groups = lax.axis_size("tok")
    signed = activations * signs.astype(jnp.bfloat16)[None, :]
    pieces, flips = [], []
    for k in range(blocks):
        piece = signed
        if k:
            piece = lax.ppermute(signed, "blk", [(i, i ^ k) for i in range(blocks)])
        pieces.append(piece)
        table = jnp.asarray([1.0 - 2.0 * parity(i & (i ^ k)) for i in range(blocks)], jnp.float32)
        flips.append(table[me])
    rotated, squares = rotate(pieces, jnp.stack(flips).reshape(1, blocks))
    row_count = FEATURES // token_groups
    window = -(-row_count // LANES) * LANES
    all_tokens, rows_window, parts = gather(rotated, squares, window, row_count)
    trace_total = jnp.sum(parts[:, 0, 0])
    diag_mean = trace_total / FEATURES + EPS
    hessian, peak = gram(rows_window, all_tokens, row_count, 1.0 / diag_mean)
    peaks = spread(peak)[:, 0, :]
    ratios = jnp.max(peaks.reshape(token_groups, blocks, row_count), axis=1).reshape(FEATURES)
    incoherence = lax.dynamic_slice_in_dim(ratios, me * block_width, block_width, 0)
    return (hessian, incoherence, jnp.max(ratios))


def solution(mesh):
    in_specs = (P("tok", "blk"), P("blk"))
    out_specs = (P("tok", "blk"), P("blk"), P())
    return jax.shard_map(
        per_device, mesh=mesh, in_specs=in_specs, out_specs=out_specs, check_vma=False
    )
```
